32 devices in a mesh: snap: 4 (over x, core), lag: 8 (over z, y).
Axes of the slice: x: 2, y: 2, z: 4, core: 2. Of those that a mesh axis runs over, the one named last changes fastest.
Arguments:
- snapshots: bfloat16 [2, 16384, 256], P(None, 'snap', 'lag')
- positions: int32 [256], replicated, may hold values from 0 to 16383, as said below
- counts: int32 [4], P('snap'), may hold values from 1 to 4096, 8192 in all
- initial: float32 [2, 96, 16384], P(None, None, 'lag'), may hold values from -6 to 6
Outputs:
- lag_corr: float32 [2, 16384], P(None, 'lag')
- subspace: float32 [2, 96, 16384], P(None, None, 'lag')
The draws below stay inside these ranges and needn't reach their ends.
Inputs may be any that keep to these rules, and one draw needn't show every extreme that they name: `positions`: positions are distinct; 0 and 16383 are among them.
All inputs are finite; a program needn't handle non-finite values. No bound on the sum of `counts` on one device may be relied on, other than what follows from the above.
Results may differ from the reference program's by a relative error of at most 0.0003.
Values may be sent and summed in bfloat16 or wider, within the bound.
No kernel may reach another device: no remote copies, remote signals or barrier semaphores. Data moves between devices by JAX's collectives and lax.ppermute only.
A program may use at most 64 MiB of HBM per device.

```python
import math
import jax
import jax.numpy as jnp
import numpy as np
from jax import lax

SENSORS = 256
LAGS = 16384
ITERS = 2
SNAP_DEV = 4096
COLUMNS = 96
N_SNAP = 4


wave_count = 128


def sensor_layout(key):
    inner = jax.random.permutation(jax.random.fold_in(key, 7), LAGS - 2)[:SENSORS - 2] + 1
    head = jnp.zeros((1,), jnp.int32)
    tail = jnp.full((1,), LAGS - 1, jnp.int32)
    return jnp.concatenate([head, inner.astype(jnp.int32), tail])


def draw_positions(key, part):
    return sensor_layout(key)


def draw_snapshots(key, part):
    placed = sensor_layout(key).astype(jnp.float32)
    keys = jax.random.split(jax.random.fold_in(key, 29), 4)
    directions = jax.random.uniform(keys[0], (wave_count,), jnp.float32, -1.0, 1.0)
    powers = jnp.exp(jax.random.uniform(keys[1], (wave_count,), jnp.float32, math.log(0.5), math.log(2.0)))
    spread = jnp.sqrt(powers / (2.0 * wave_count))
    amplitude = jax.random.normal(keys[2], (2, SNAP_DEV * N_SNAP, wave_count), jnp.float32)
    noise_level = 0.3
    amplitude = amplitude * spread[None, None, :]
    phase = math.pi * placed[:, None] * directions[None, :]
    cosine = jnp.cos(phase)
    sine = jnp.sin(phase)
    real_part = amplitude[0] @ cosine.T - amplitude[1] @ sine.T
    imag_part = amplitude[0] @ sine.T + amplitude[1] @ cosine.T
    noise = noise_level * jax.random.normal(keys[3], (2, SNAP_DEV * N_SNAP, SENSORS), jnp.float32)
    return (jnp.stack([real_part, imag_part]) + noise).astype(jnp.bfloat16)


def block_scale(stream_key, extent, cuts, smallest, high):
    level, own = 1.0, jax.random.fold_in(stream_key, 6)
    for position, parts in cuts:
        draws = jnp.exp(jax.random.uniform(jax.random.fold_in(own, position), (parts,), jnp.float32, smallest / len(cuts), high / len(cuts)))
        level = level * jnp.repeat(draws, extent[position] // parts).reshape([-1 if axis == position else 1 for axis in range(len(extent))])
    return level


def length_profile(amount, total, limit, slope):
    weights = [(1 << 20) // math.isqrt(grade ** slope) + 1 for grade in range(2, amount + 1)]
    rest, given = total - limit - (amount - 1), [1] * (amount - 1)
    while rest > 0:
        candidates = [i for i in range(amount - 1) if given[i] < limit]
        pool, budget = sum([weights[i] for i in candidates]), rest
        for i in candidates:
            addition = min(limit - given[i], max(1, budget * weights[i] // pool), rest)
            given[i] = given[i] + addition
            rest = rest - addition
    return np.array([limit] + given)


def ragged(key, amount, total, most, slope):
    if amount == 2:
        one = jax.random.randint(key, (), max(1, total - most), min(most, total - 1) + 1)
        return jnp.stack([one, total - one])
    lengths = jnp.asarray(length_profile(amount, total, most, slope), jnp.int32)
    pairs = (amount - 1) // 2
    giver, receiver = lengths[1:1 + 2 * pairs:2], lengths[2:2 + 2 * pairs:2]
    room = jnp.minimum(giver - 1, most - receiver)
    moved = jax.random.randint(jax.random.fold_in(key, 1), (pairs,), 0, 1 << 20) % (room + 1)
    lengths = lengths.at[1:1 + 2 * pairs:2].set(giver - moved).at[2:2 + 2 * pairs:2].set(receiver + moved)
    return lengths[jax.random.permutation(jax.random.fold_in(key, 2), amount)]


def normal_values(stream_key, dims, scale, reach, pieces=(), kind=jnp.bfloat16):
    values = scale * jax.random.normal(stream_key, dims, jnp.float32)
    if pieces:
        values = values * block_scale(stream_key, dims, pieces, -0.22, 0.18)
    return jnp.clip(values, -reach, reach).astype(kind)


def setup_inputs(seed: int = 0) -> dict:
    streams_of = jax.random.split(jax.random.key(seed), 5)
    snapshots = draw_snapshots(jax.random.fold_in(streams_of[4], 71), 0)
    positions = draw_positions(jax.random.fold_in(streams_of[4], 71), 0)
    counts = ragged(streams_of[2], N_SNAP, SNAP_DEV * N_SNAP // 2, SNAP_DEV, 2).astype(jnp.int32)
    initial = normal_values(streams_of[3], (2, COLUMNS, LAGS), 1.0, 6.0, ((2, 8),), jnp.float32)
    return {"snapshots": snapshots, "positions": positions, "counts": counts, "initial": initial}


exact = lax.Precision.HIGHEST

def correlate(former, latter):

    def product(left_rows, right_rows):
        return jnp.dot(left_rows.T.astype(jnp.float32), right_rows.astype(jnp.float32), preferred_element_type=jnp.float32)
    real_part = product(former[0], latter[0]) + product(former[1], latter[1])
    imag_part = product(former[1], latter[0]) - product(former[0], latter[1])
    return (real_part, imag_part)

def toeplitz_apply(columns, spectrum):
    complex_columns = columns[0] + 1j * columns[1]
    transformed = jnp.fft.fft(complex_columns, n=2 * LAGS, axis=1)
    mapped = jnp.fft.ifft(transformed * spectrum[None, :], axis=1)[:, :LAGS]
    return jnp.stack([jnp.real(mapped), jnp.imag(mapped)])

def reference(snapshots, positions, counts, initial):
    row_ids = jnp.arange(snapshots.shape[1], dtype=jnp.int32)
    live_rows = row_ids % SNAP_DEV < counts[row_ids // SNAP_DEV]
    masked = jnp.where(live_rows[None, :, None], snapshots, jnp.zeros((), snapshots.dtype))
    corr_real, corr_imag = correlate(masked, masked)
    pair_lags = positions[:, None] - positions[None, :]
    usable = pair_lags >= 0
    pair_bins = jnp.where(usable, pair_lags, LAGS).reshape(-1).astype(jnp.int32)

    def binned(values):
        return jax.ops.segment_sum(values.reshape(-1), pair_bins, num_segments=LAGS + 1)[:LAGS]
    pair_count = binned(usable.astype(jnp.float32))
    snap_total = jnp.sum(counts).astype(jnp.float32)
    divisor = jnp.maximum(pair_count, 1.0) * snap_total
    lag_corr = jnp.stack([binned(corr_real) / divisor, binned(corr_imag) / divisor])
    halves = jnp.where(jnp.arange(LAGS) == 0, 0.5, 1.0).astype(jnp.float32)
    weighted = lag_corr[0] * halves + 1j * (lag_corr[1] * halves)
    spectrum = 2.0 * jnp.real(jnp.fft.fft(weighted, n=2 * LAGS))
    columns = initial
    for sweep in range(ITERS):
        mapped = toeplitz_apply(columns, spectrum)
        gram_matrix = jnp.einsum('xaj,xbj->ab', mapped, mapped, precision=exact) / LAGS
        factor = jnp.linalg.cholesky(gram_matrix)
        identity = jnp.eye(gram_matrix.shape[0], dtype=gram_matrix.dtype)
        inverse = lax.linalg.triangular_solve(factor, identity, left_side=True, lower=True)
        columns = jnp.einsum('ab,xbj->xaj', inverse, mapped, precision=exact)
    return (lag_corr, columns)
```

```python
import math

import jax
import jax.numpy as jnp
import ml_dtypes
import numpy as np
from jax import lax
from jax.experimental import pallas as pl
from jax.experimental.pallas import tpu as pltpu
from jax.sharding import PartitionSpec as P

ITERS = 2
LANES = 128
LOW = 64

f32 = jnp.float32
bf16 = jnp.bfloat16
VMEM = pl.BlockSpec(memory_space=pltpu.VMEM)
SMEM = pl.BlockSpec(memory_space=pltpu.SMEM)
NT = (((1,), (1,)), ((), ()))


def split_table(table):
    high = table.astype(np.float32).astype(ml_dtypes.bfloat16)
    low = (table - high.astype(np.float64)).astype(np.float32).astype(ml_dtypes.bfloat16)
    return np.stack([high, low])


def tables(length):
    padded = 2 * length
    first = padded // LANES
    half = first // 2
    k, t = np.arange(first)[:, None], np.arange(half)[None, :]
    angle = 2.0 * np.pi * (k * t % first) / first
    cosine, sine = np.cos(angle), np.sin(angle)
    outer = np.block([[cosine, sine], [-sine, cosine]])
    s = np.arange(LANES)
    angle = 2.0 * np.pi * (s[:, None] * s[None, :] % LANES) / LANES
    cosine, sine = np.cos(angle), np.sin(angle)
    inner = np.block([[cosine, -sine], [sine, cosine]])
    angle = 2.0 * np.pi * (k * s[None, :] % padded) / padded
    twist = np.stack([np.cos(angle), np.sin(angle)]).astype(np.float32)
    return (split_table(outer), split_table(inner), split_table(inner.T), split_table(outer.T), twist)


def halves(values):
    high = values.astype(bf16)
    return high, (values - high.astype(f32)).astype(bf16)


def dot(left, right):
    return jnp.dot(left, right, preferred_element_type=f32)


def table_left(table, values):
    high, low = halves(values)
    return dot(table[0], high) + (dot(table[0], low) + dot(table[1], high))


def table_right(values, table):
    high, low = halves(values)
    return dot(high, table[0]) + (dot(low, table[0]) + dot(high, table[1]))


def corr_bins_kernel(x_ref, pos_ref, share_ref, out_ref, hi_ref, lo_ref, v_ref):
    groups, _, here, slots = x_ref.shape
    sensors = groups * here
    half = sensors // 2
    high_count = out_ref.shape[0]
    real = x_ref[:, 0].astype(f32).reshape(sensors, slots).astype(bf16)
    imag = x_ref[:, 1].astype(f32).reshape(sensors, slots).astype(bf16)
    i = lax.broadcasted_iota(jnp.int32, (sensors, sensors), 0)
    k = lax.broadcasted_iota(jnp.int32, (sensors, sensors), 1)
    mirror = i + k == sensors - 1
    flip = jnp.where(mirror, 1.0, 0.0).astype(bf16)

    def products(re, im):
        def outer(a, b):
            return lax.dot_general(a[:half], b, NT, preferred_element_type=f32)

        return outer(re, re) + outer(im, im), outer(im, re) - outer(re, im)

    front = products(real, imag)
    back = products(dot(flip, real).astype(bf16), dot(flip, imag).astype(bf16))
    pos = pos_ref[...].astype(f32)
    col = jnp.sum(jnp.where(i == k, pos, 0.0), axis=1, keepdims=True)
    back_col = jnp.sum(jnp.where(mirror, pos, 0.0), axis=1, keepdims=True)
    back_row = jnp.sum(jnp.where(mirror, col, 0.0), axis=0, keepdims=True)
    below, above, same = (k < i)[:half], (k > i)[:half], (k == i)[:half]
    diff = jnp.where(below, col[:half] - pos, back_col[:half] - back_row)
    lags = jnp.abs(diff).astype(jnp.int32)
    hi_ref[...] = lags // LOW
    lo_ref[...] = lags % LOW
    re = jnp.where(below, front[0], jnp.where(above, back[0], 0.0))
    im = jnp.where(below, front[1], jnp.where(above, back[1], 0.0))
    im = jnp.where(diff >= 0.0, im, -im)
    trace = jnp.sum(jnp.where(same, front[0] + back[0], 0.0))
    for plane, value in enumerate((re, im)):
        high = value.astype(bf16).astype(f32)
        v_ref[plane] = high
        v_ref[plane + 2] = value - high
    high_ids = lax.broadcasted_iota(jnp.int32, (high_count, sensors), 0)
    low_ids = lax.broadcasted_iota(jnp.int32, (LOW, sensors), 0)
    unroll = math.gcd(half, 8)

    def accumulate(block, acc):
        left, right = [], []
        for u in range(unroll):
            row = pl.ds(block * unroll + u, 1)
            left.append(jnp.where(high_ids == hi_ref[row, :], 1.0, 0.0).astype(bf16))
            hot = low_ids == lo_ref[row, :]
            right.append(
                jnp.concatenate([jnp.where(hot, v_ref[p, row, :], 0.0) for p in range(4)], 0).astype(bf16)
            )
        return acc + lax.dot_general(
            jnp.concatenate(left, 1), jnp.concatenate(right, 1), NT, preferred_element_type=f32
        )

    acc = lax.fori_loop(0, half // unroll, accumulate, jnp.zeros((high_count, 4 * LOW), f32))
    out = acc[:, : 2 * LOW] + acc[:, 2 * LOW :]
    row = lax.broadcasted_iota(jnp.int32, out.shape, 0)
    lane = lax.broadcasted_iota(jnp.int32, out.shape, 1)
    out = out + jnp.where((row == 0) & (lane == 0), trace, 0.0)
    out_ref[...] = jnp.where((row == 0) & (lane == LOW), share_ref[0, 0], out)


def sum_spread_kernel(in_ref, out_ref):
    out_ref[...] = jnp.broadcast_to(jnp.sum(in_ref[...], axis=0, keepdims=True), out_ref.shape)


def operator_kernel(
    bins_ref, cols_ref, pos_ref, outer_ref, inner_ref, inner_t_ref, outer_t_ref, twist_ref, lag_ref, out_ref, y_ref
):
    blocks, _, count, rows, _ = cols_ref.shape
    half = blocks * rows
    first = 2 * half
    cosine, sine = twist_ref[0], twist_ref[1]

    def piece(values, j):
        return values[:, j * LANES : (j + 1) * LANES]

    def forward(values, n):
        spread = table_left(outer_ref, values)
        rows_out = []
        for j in range(n):
            part = piece(spread, j)
            re, im = part[:first], part[first:]
            rows_out.append(jnp.concatenate([cosine * re + sine * im, cosine * im - sine * re], 1))
        return table_right(jnp.concatenate(rows_out, 0), inner_ref)

    def backward(values, n):
        spread = table_right(values, inner_t_ref)
        cols_out = []
        for j in range(n):
            part = spread[j * first : (j + 1) * first]
            re, im = part[:, :LANES], part[:, LANES:]
            cols_out.append(jnp.concatenate([cosine * re - sine * im, cosine * im + sine * re], 0))
        return table_left(outer_t_ref, jnp.concatenate(cols_out, 1))

    pos = pos_ref[...]
    sensors = pos.shape[1]
    t_ids = lax.broadcasted_iota(jnp.int32, (half, sensors), 0)
    s_ids = lax.broadcasted_iota(jnp.int32, (LANES, sensors), 0)
    placed = lax.dot_general(
        jnp.where(t_ids == pos // LANES, 1.0, 0.0).astype(bf16),
        jnp.where(s_ids == pos % LANES, 1.0, 0.0).astype(bf16),
        NT,
        preferred_element_type=f32,
    )
    columns = [
        jnp.concatenate([cols_ref[:, 0, j].reshape(half, LANES), cols_ref[:, 1, j].reshape(half, LANES)], 0)
        for j in range(count)
    ]
    placed = jnp.concatenate([placed, jnp.zeros_like(placed)], 0)
    spectra = forward(jnp.concatenate(columns + [placed], 1), count + 1)
    power = spectra[count * first :]
    power = power[:, :LANES] ** 2 + power[:, LANES:] ** 2
    pairs = backward(jnp.concatenate([power, jnp.zeros_like(power)], 1), 1)[:half]
    pairs = jnp.round(pairs * (1.0 / (first * LANES)))

    even = bins_ref[pl.ds(0, half, stride=2), :]
    odd = bins_ref[pl.ds(1, half, stride=2), :]
    lane = lax.broadcasted_iota(jnp.int32, even.shape, 1)
    row = lax.broadcasted_iota(jnp.int32, even.shape, 0)
    re = jnp.where(lane < LOW, even, pltpu.roll(odd, LOW, 1))
    im = jnp.where(lane < LOW, pltpu.roll(even, LOW, 1), odd)
    origin = (row == 0) & (lane == 0)
    total = im[0:1, 0:1]
    im = jnp.where(origin, 0.0, im)
    divisor = jnp.maximum(pairs, 1.0) * total
    re, im = re / divisor, im / divisor
    lag_ref[0] = re
    lag_ref[1] = im
    level = re[0:1, 0:1]
    weight = jnp.where(origin, 0.5, 1.0)
    spectrum = forward(jnp.concatenate([re * weight, im * weight], 0) / level, 1)[:, :LANES]
    spectrum = spectrum * (2.0 / (first * LANES))
    spectrum = jnp.concatenate([spectrum, spectrum], 1)
    spectrum = jnp.concatenate([spectrum] * count, 0)
    image = backward(spectra[: count * first] * spectrum, count)
    for sweep in range(1, ITERS):
        image = backward(forward(image, count) * spectrum, count)
    y_ref[...] = image
    chunks, _, _, depth, _ = out_ref.shape
    for chunk in range(chunks):
        for x in range(2):
            for j in range(count):
                out_ref[chunk, x, j] = y_ref[
                    pl.ds(x * half + chunk * depth, depth), j * LANES : (j + 1) * LANES
                ]


def call(kernel, out_shape, *args, scratch=(), in_specs=None):
    return pl.pallas_call(
        kernel,
        out_shape=out_shape,
        in_specs=in_specs or [VMEM] * len(args),
        out_specs=jax.tree.map(lambda _: VMEM, out_shape),
        scratch_shapes=list(scratch),
    )(*args)


def shape_of(*dims):
    return jax.ShapeDtypeStruct(dims, f32)


def gather_columns(block_ref, count, depth, sources):
    parts = []
    for x in range(2):
        for r in range(depth):
            parts.append(
                jnp.concatenate(
                    [
                        block_ref[pl.ds((x * count + j) * depth + r, sources, stride=2 * count * depth), :]
                        for j in range(count)
                    ],
                    0,
                )
            )
    return jnp.concatenate(parts, 1)


def on_device(snapshots, positions, counts, initial):
    lag_size, snap_size = lax.axis_size("lag"), lax.axis_size("snap")
    lag_index, snap_index = lax.axis_index("lag"), lax.axis_index("snap")
    rows_here, sensors_here = snapshots.shape[1:]
    column_total, lag_dev = initial.shape[1:]
    lag_total = lag_dev * lag_size
    devices = lag_size * snap_size
    both = ("snap", "lag")
    shared = column_total % devices == 0
    sources = devices if shared else lag_size
    group = both if shared else "lag"
    parts = snap_size if shared else 1
    count = column_total // sources
    depth = lag_dev // parts // LANES
    table_args = [jnp.asarray(t) for t in tables(lag_total)]

    mine = initial.reshape(2, count, parts, lag_size, lag_dev // LANES, LANES)
    mine = lax.dynamic_index_in_dim(mine, snap_index if shared else 0, 2, keepdims=False)
    mine = lax.all_to_all(jnp.transpose(mine, (2, 0, 1, 3, 4)), "lag", 0, 0, tiled=True)

    live = jnp.arange(rows_here, dtype=jnp.int32) < counts[0]
    masked = jnp.where(live[None, :, None], snapshots, jnp.zeros((), snapshots.dtype))
    slots = rows_here // lag_size
    sent = jnp.transpose(masked.reshape(2, lag_size, slots, sensors_here), (1, 0, 3, 2))
    seen = lax.all_to_all(sent, "lag", 0, 0, tiled=True)

    pos_row = positions.reshape(1, -1)
    sensors = positions.shape[0]
    share = jnp.where(lag_index == 0, counts, 0).astype(f32).reshape(1, 1)
    high_count = lag_total // LOW
    bins = call(
        corr_bins_kernel,
        shape_of(high_count, 2 * LOW),
        seen,
        pos_row,
        share,
        scratch=[
            pltpu.VMEM((sensors // 2, sensors), jnp.int32),
            pltpu.VMEM((sensors // 2, sensors), jnp.int32),
            pltpu.VMEM((4, sensors // 2, sensors), f32),
        ],
        in_specs=[VMEM, VMEM, SMEM],
    )
    split = (devices, high_count // devices, 2 * LOW)
    bins = lax.all_to_all(bins.reshape(split), both, 0, 0, tiled=True)
    bins = call(sum_spread_kernel, shape_of(*split), bins)
    bins = lax.all_to_all(bins, both, 0, 0, tiled=True).reshape(high_count, 2 * LOW)

    lag_rows = lag_total // LANES
    lag_all, image = call(
        operator_kernel,
        (shape_of(2, lag_rows, LANES), shape_of(lag_size * parts, 2, count, depth, LANES)),
        bins,
        mine,
        pos_row,
        *table_args,
        scratch=[pltpu.VMEM((2 * lag_rows, count * LANES), f32)],
    )
    here = lag_dev // LANES
    lag_corr = lax.dynamic_slice_in_dim(lag_all, lag_index * here, here, 1).reshape(2, lag_dev)

    block = 2 * count * depth
    image = image.reshape(lag_size, parts, block, LANES)
    image = jnp.swapaxes(image, 0, 1).reshape(sources, block, LANES)
    image = lax.all_to_all(image, group, 0, 0, tiled=True).reshape(sources * block, LANES)

    def gram(in_ref, out_ref):
        matrix = gather_columns(in_ref, count, depth, sources)
        out_ref[...] = lax.dot_general(
            matrix, matrix, NT, precision=lax.Precision.HIGHEST, preferred_element_type=f32
        ) * (1.0 / lag_total)

    total = call(gram, shape_of(column_total, column_total), image)
    for axis, size in (("lag", lag_size),) + ((("snap", snap_size),) if shared else ()):
        step = 1
        while step < size:
            total = total + lax.ppermute(total, axis, [(d, d ^ step) for d in range(size)])
            step *= 2

    held = [image]
    if shared:
        step = 1
        while step < snap_size:
            held = held + [
                lax.ppermute(h, "snap", [(d, d ^ step) for d in range(snap_size)]) for h in held
            ]
            step *= 2

    def finish(*refs):
        where_ref, gram_ref, *rest = refs
        blocks, out_ref = rest[:-1], rest[-1]
        n = column_total
        row = lax.broadcasted_iota(jnp.int32, (n, 2 * LANES), 0)
        lane = lax.broadcasted_iota(jnp.int32, (n, 2 * LANES), 1)
        work = jnp.concatenate(
            [gram_ref[...], jnp.zeros((n, LANES - n), f32), jnp.zeros((n, LANES), f32)], 1
        )
        work = jnp.where(lane == row + LANES, 1.0, work)
        for j in range(n):
            pivot_row = work[j : j + 1, :]
            column = work[:, j : j + 1]
            factor = jnp.where(row[:, :1] > j, column / work[j : j + 1, j : j + 1], 0.0)
            work = work - factor * pivot_row
        diagonal = jnp.sum(jnp.where(lane == row, work, 0.0), axis=1, keepdims=True)
        inverse = work[:, LANES : LANES + n] * lax.rsqrt(diagonal)
        for position, block_ref in enumerate(blocks):
            matrix = gather_columns(block_ref, count, depth, sources)
            result = jnp.dot(inverse, matrix, precision=lax.Precision.HIGHEST, preferred_element_type=f32)
            width = depth * LANES
            start = (where_ref[0] ^ position) * width
            for x in range(2):
                out_ref[x, :, pl.ds(pl.multiple_of(start, LANES), width)] = result[
                    :, x * width : (x + 1) * width
                ]

    where = (snap_index if shared else jnp.zeros((), jnp.int32)).astype(jnp.int32).reshape(1)
    subspace = call(
        finish,
        shape_of(2, column_total, lag_dev),
        where,
        total,
        *held,
        in_specs=[SMEM] + [VMEM] * (1 + len(held)),
    )
    return (lag_corr, subspace)


def solution(mesh):
    return jax.shard_map(
        on_device,
        mesh=mesh,
        in_specs=(P(None, "snap", "lag"), P(), P("snap"), P(None, None, "lag")),
        out_specs=(P(None, "lag"), P(None, None, "lag")),
        check_vma=False,
    )
```
